32 devices in a mesh: grp: 8 (over y, x, core), blk: 4 (over z).
Axes of the slice: x: 2, y: 2, z: 4, core: 2. Of those that a mesh axis runs over, the one named last changes fastest.
Arguments:
- visual: bfloat16 [24576, 3584], P(('grp', 'blk')), may hold values from -6 to 6
- text_queries: float32 [1024, 3584], P(('grp', 'blk')), may hold values from -100 to 100
- kv_weight: bfloat16 [3584, 1024], replicated, may hold values from -0.09375 to 0.09375
- placement: int32 [3072, 1], P(('grp', 'blk')), may hold values from 0 to 31; in each aligned block of 96 rows (0 to 95, 96 to 191, ...) at most 4 rows name the same one
Outputs:
- attended: float32 [1024, 3584], P(('grp', 'blk'))
The draws below stay inside these ranges and needn't reach their ends.
Inputs may be any that keep to these rules, and one draw needn't show every extreme that they name: `placement`: among the 96 blocks of one frame owner at most 4 name the same attention owner, a bound that some block reaches; every attention owner is named by some block.
All inputs are finite; a program needn't handle non-finite values.
Results may differ from the reference program's by a relative error of at most 0.0003.
Values sent between devices are 32-bit elements; how exact they have to be, the bound alone decides.
A program may use at most 128 MiB of HBM per device.

```python
import math
import jax
import jax.numpy as jnp
import numpy as np
from jax import lax

DV = 3584
HEADS = 28
KV_HEADS = 4
HEAD_DIM = 128
QROWS = 32
BLOCKS = 96
BLOCK_ROWS = 8
PER_PAIR = 4
TEXT = 1024
VISUAL = 24576
N_GRP = 8
N_BLK = 4
DEVICES = 32


def draw_text_queries(key, part):
    base = jax.random.normal(key, (TEXT, HEADS * HEAD_DIM), jnp.float32)
    return jnp.clip(base, -100.0, 100.0)


def shard_levels(rng, shape, cuts, smallest, largest):
    gain = 1.0
    for dim, blocks in cuts:
        draws = jax.random.uniform(jax.random.fold_in(jax.random.fold_in(rng, 6), dim), (blocks,), jnp.float32, smallest / len(cuts), largest / len(cuts))
        gain = gain * jnp.repeat(jnp.exp(draws), shape[dim] // blocks).reshape((-1,) + (1,) * (len(shape) - 1 - dim))
    return gain


def assign_block(rng, own, number, rows, number_of, top, bound, skew):
    sequence = jax.random.permutation(rng, number_of)
    packed, common = portions_of(number_of, rows * top, bound, skew, True), portions_of(number_of, rows * top, bound, skew, False)
    places = jnp.arange(number_of)

    def named(sizes, rotation):
        used = int((sizes > 0).sum())
        fixed = max(1, used // 4)
        shifted = fixed + (places - fixed + rotation * (used - fixed)) % max(1, number_of - fixed)
        return jnp.zeros((number_of,), jnp.int32).at[sequence[jnp.where(places < fixed, places, shifted)]].set(jnp.asarray(sizes, jnp.int32))

    sizes = jnp.where(number % 4 == 0, named(packed, number // 4), named(common, number - number // 4 - 1))
    mixed = jax.random.permutation(jax.random.fold_in(own, 3), number_of)
    source_of, taker = mixed[0:number_of // 2 * 2:2], mixed[1:number_of // 2 * 2:2]
    slack = jnp.minimum(sizes[source_of] - 1, bound - sizes[taker]) // 2
    slack = jnp.where((source_of == sequence[0]) | (taker == sequence[0]) | (sizes[taker] == 0), 0, jnp.maximum(slack, 0))
    shifted = jax.random.randint(jax.random.fold_in(own, 4), (number_of // 2,), 0, 1 << 20) % (slack + 1)
    sizes = sizes.at[source_of].add(-shifted).at[taker].add(shifted)
    labels = jnp.searchsorted(jnp.cumsum(sizes), jnp.arange(rows * top), side="right").astype(jnp.int32)
    table = labels.reshape(top, rows).T
    table = table[jax.random.permutation(jax.random.fold_in(own, 1), rows)]
    rotation = jax.random.randint(jax.random.fold_in(own, 2), (rows, 1), 0, top)
    return jnp.take_along_axis(table, (jnp.arange(top)[None, :] + rotation) % top, axis=1)


def portions_of(number_of, total, most, skew, full):
    loads = [(1 << 20) // math.isqrt(rank ** skew) + 1 for rank in range(1, number_of + 1)]
    largest = most if full else min(most, max(-(-total // number_of), total * loads[0] // sum(loads)))
    least = 1 if total - largest >= number_of - 1 else 0
    holding, surplus = [largest] + [least] * (number_of - 1), total - largest - least * (number_of - 1)
    while surplus > 0:
        movable = [i for i in range(1, number_of) if holding[i] < largest] or [i for i in range(1, number_of) if holding[i] < most]
        pool, left = sum([loads[i] for i in movable]), surplus
        for i in movable:
            more = min(most - holding[i], max(1, left * loads[i] // pool), surplus)
            holding[i] = holding[i] + more
            surplus = surplus - more
    return np.array(holding)


def scatter_about(own_key, extent, scale, most, pieces=(), kind=jnp.bfloat16):
    factor_of = shard_levels(own_key, extent, pieces, -0.22, 0.18) if pieces else 1.0
    entries = jax.random.normal(own_key, extent, jnp.float32) * scale * factor_of
    return jnp.minimum(jnp.maximum(entries, -most), most).astype(kind)


def setup_inputs(seed: int = 0) -> dict:
    key_of = jax.random.split(jax.random.key(seed), 5)
    visual = scatter_about(key_of[0], (VISUAL, DV), 1.0, 6.0, ((0, 32),))
    text_queries = draw_text_queries(jax.random.fold_in(key_of[4], 71), 0)
    kv_weight = scatter_about(key_of[2], (DV, 2 * KV_HEADS * HEAD_DIM), DV ** -0.5, 0.09375)
    placement_keys = jax.random.split(jax.random.fold_in(key_of[3], 1), (BLOCKS * DEVICES) // BLOCKS)
    placement_turns = jax.random.permutation(jax.random.fold_in(key_of[3], 3), (BLOCKS * DEVICES) // BLOCKS)
    placement = jax.vmap(lambda own, number: assign_block(jax.random.fold_in(key_of[3], 2), own, number, BLOCKS, DEVICES, 1, PER_PAIR, 2))(placement_keys, placement_turns).reshape((BLOCKS * DEVICES, 1))
    return dict(visual=visual, text_queries=text_queries, kv_weight=kv_weight, placement=placement)


def reference(visual, text_queries, kv_weight, placement):
    devices = N_GRP * N_BLK
    group = HEADS // KV_HEADS
    width = 2 * KV_HEADS * HEAD_DIM
    kv = jnp.dot(visual, kv_weight, preferred_element_type=jnp.float32)
    flat_blocks = kv.reshape(devices * BLOCKS, BLOCK_ROWS * width)
    owner = placement.reshape(devices, BLOCKS).astype(jnp.int32)
    index = jnp.arange(BLOCKS, dtype=jnp.int32)
    earlier = (owner[:, :, None] == owner[:, None, :]) & (index[None, None, :] < index[None, :, None])
    rank = jnp.sum(earlier.astype(jnp.int32), axis=2, dtype=jnp.int32)
    source = jnp.arange(devices, dtype=jnp.int32)[:, None]
    slot = owner * (devices * PER_PAIR) + source * PER_PAIR + rank
    span = N_BLK * devices * PER_PAIR
    scale = HEAD_DIM ** -0.5

    def segment(seg):
        local = slot - seg * span
        inside = (local >= 0) & (local < span)
        target = jnp.where(inside, local, span).reshape(-1).astype(jnp.int32)
        buffer = jnp.zeros((span, BLOCK_ROWS * width), jnp.float32).at[target].set(flat_blocks, mode="drop")
        marks = jnp.zeros((span, BLOCK_ROWS), jnp.float32).at[target].set(1.0, mode="drop")
        keys_all = buffer.reshape(span * BLOCK_ROWS, width)
        valid = marks.reshape(-1) > 0.5
        key_heads = keys_all[:, :KV_HEADS * HEAD_DIM].reshape(-1, KV_HEADS, HEAD_DIM)
        value_heads = keys_all[:, KV_HEADS * HEAD_DIM:].reshape(-1, KV_HEADS, HEAD_DIM)
        rows = lax.dynamic_slice_in_dim(text_queries, seg * N_BLK * QROWS, N_BLK * QROWS, 0)
        query_heads = rows.reshape(-1, KV_HEADS, group, HEAD_DIM)
        scores = jnp.einsum("rgjd,kgd->rgjk", query_heads, key_heads, precision=lax.Precision.HIGHEST) * scale
        scores = jnp.where(valid[None, None, None, :], scores, -1e30)
        weights = jax.nn.softmax(scores, axis=-1)
        result = jnp.einsum("rgjk,kgd->rgjd", weights, value_heads, precision=lax.Precision.HIGHEST)
        return result.reshape(N_BLK * QROWS, HEADS * HEAD_DIM)

    results = lax.map(segment, jnp.arange(N_GRP, dtype=jnp.int32))
    return results.reshape(TEXT, HEADS * HEAD_DIM)
```

```python
import functools

import jax
import jax.numpy as jnp
from jax import lax
from jax.experimental import pallas as pl
from jax.experimental.pallas import tpu as pltpu
from jax.sharding import PartitionSpec as P

HEADS = 28
KV_HEADS = 4
MESH = pl.DeviceIdType.MESH
F32 = jnp.float32
BF16 = jnp.bfloat16
NT = (((1,), (1,)), ((), ()))


def dot(a, b):
    return jnp.dot(a, b, preferred_element_type=F32)


def split3(x):
    hi = x.astype(BF16)
    rest = x - hi.astype(F32)
    mid = rest.astype(BF16)
    low = (rest - mid.astype(F32)).astype(BF16)
    return hi, mid, low


def kernel(
    n_grp, n_blk, per_seg, group, dim,
    visual_hbm, query_hbm, weight_hbm, place_ref,
    out_ref,
    visual, weight, pieces, outgoing, arrived, queries,
    counts_out, counts_in, bias, kcat_a, kcat_b, v_t, p_hi, p_lo,
    stats_out, stats_in, partial, partial_in,
    load_sem, weight_sem, query_load_sem,
    query_send, query_recv, count_send, count_recv,
    kv_send, kv_recv, stat_send, stat_recv, part_send, part_recv,
):
    me_g = lax.axis_index("grp")
    me_b = lax.axis_index("blk")
    rows = query_hbm.shape[0]
    n_rows = visual.shape[0]
    blocks = place_ref.shape[0]
    block_rows = n_rows // blocks
    seg_rows = per_seg * block_rows
    lanes = n_blk * rows
    kv_heads = KV_HEADS
    scale = dim ** (-0.5)

    query_load = pltpu.make_async_copy(query_hbm, queries.at[me_b], query_load_sem)
    query_load.start()
    visual_load = pltpu.make_async_copy(visual_hbm, visual, load_sem)
    visual_load.start()

    def weight_loads(h):
        slot = h % 2
        return [
            pltpu.make_async_copy(
                weight_hbm.at[:, pl.ds((half * kv_heads + h) * dim, dim)],
                weight.at[slot, :, pl.ds(half * dim, dim)],
                weight_sem.at[slot, half],
            )
            for half in range(2)
        ]

    for h in range(2):
        for copy in weight_loads(h):
            copy.start()

    barrier = pltpu.get_barrier_semaphore()
    for d in range(1, n_grp):
        pl.semaphore_signal(
            barrier, inc=1, device_id={"grp": lax.rem(me_g + d, n_grp)}, device_id_type=MESH
        )
    for e in range(1, n_blk):
        pl.semaphore_signal(
            barrier, inc=1, device_id={"blk": lax.rem(me_b + e, n_blk)}, device_id_type=MESH
        )
    pl.semaphore_wait(barrier, n_grp + n_blk - 2)

    query_load.wait()
    query_copies = []
    for e in range(1, n_blk):
        copy = pltpu.make_async_remote_copy(
            src_ref=queries.at[me_b],
            dst_ref=queries.at[me_b],
            send_sem=query_send.at[e],
            recv_sem=query_recv.at[e],
            device_id={"blk": lax.rem(me_b + e, n_blk)},
            device_id_type=MESH,
        )
        copy.start()
        query_copies.append(copy)

    owner = place_ref[...]
    seg = jnp.zeros_like(owner)
    for g in range(1, n_grp):
        seg += (owner >= g * n_blk).astype(jnp.int32)
    block_id = lax.broadcasted_iota(jnp.int32, (blocks, n_rows), 0)
    row_id = lax.broadcasted_iota(jnp.int32, (blocks, n_rows), 1)
    first = block_id * block_rows
    within = (row_id >= first) & (row_id < first + block_rows)
    before = row_id >= first + block_rows
    seg_wide = jnp.broadcast_to(seg, (blocks, n_rows))
    row_seg = jnp.sum(jnp.where(within, seg_wide, 0), axis=0, keepdims=True)
    row_in = jnp.sum(jnp.where(within, row_id - first, 0), axis=0, keepdims=True)
    rank = jnp.sum(
        jnp.where(before & (seg_wide == row_seg), 1, 0), axis=0, keepdims=True
    )
    row_slot = row_seg * seg_rows + rank * block_rows + row_in

    for g in range(n_grp):
        count = jnp.sum((seg == g).astype(F32), axis=0, keepdims=True) * block_rows
        counts_out[g] = jnp.broadcast_to(count, counts_out.shape[1:])

    kv_copies = []
    count_copies = []
    visual_load.wait()
    tile = min(256, n_rows)
    for h in range(kv_heads):
        for copy in weight_loads(h):
            copy.wait()

        def project(i, _, slot=h % 2):
            at = pl.ds(pl.multiple_of(i * tile, tile), tile)
            hi, mid, low = split3(dot(visual[at, :], weight[slot]))
            pieces[at, 0 : 2 * dim] = hi
            pieces[at, 2 * dim : 4 * dim] = mid
            pieces[at, 4 * dim : 6 * dim] = low
            return 0

        lax.fori_loop(0, n_rows // tile, project, 0)
        if h + 2 < kv_heads:
            for copy in weight_loads(h + 2):
                copy.start()

        def pack(g, _, h=h):
            slot_id = lax.broadcasted_iota(jnp.int32, (seg_rows, n_rows), 0) + g * seg_rows
            pick = jnp.where(slot_id == row_slot, 1.0, 0.0).astype(BF16)
            both = dot(pick, pieces[...])
            both = both[:, : 2 * dim] + both[:, 2 * dim : 4 * dim] + both[:, 4 * dim :]
            outgoing[2 * h, g] = both[:, :dim]
            outgoing[2 * h + 1, g] = both[:, dim:]
            return 0

        lax.fori_loop(0, n_grp, pack, 0)
        for half in range(2):
            unit = 2 * h + half
            row = []
            for d in range(1, n_grp):
                peer = lax.rem(me_g + d, n_grp)
                copy = pltpu.make_async_remote_copy(
                    src_ref=outgoing.at[unit, peer],
                    dst_ref=arrived.at[unit, d],
                    send_sem=kv_send.at[unit, d],
                    recv_sem=kv_recv.at[unit, d],
                    device_id={"grp": peer},
                    device_id_type=MESH,
                )
                copy.start()
                row.append(copy)
            kv_copies.append(row)
            arrived[unit, 0] = outgoing[unit, me_g]
        if h == 0:
            for d in range(1, n_grp):
                peer = lax.rem(me_g + d, n_grp)
                copy = pltpu.make_async_remote_copy(
                    src_ref=counts_out.at[peer],
                    dst_ref=counts_in.at[d],
                    send_sem=count_send.at[d],
                    recv_sem=count_recv.at[d],
                    device_id={"grp": peer},
                    device_id_type=MESH,
                )
                copy.start()
                count_copies.append(copy)
            counts_in[0] = counts_out[me_g]

    for copy in query_copies:
        copy.wait_recv()
    for copy in count_copies:
        copy.wait_recv()
    key_id = lax.broadcasted_iota(jnp.int32, (seg_rows, 128), 0).astype(F32)
    for d in range(n_grp):
        bias[d * seg_rows : (d + 1) * seg_rows, :] = jnp.where(
            key_id < counts_in[d][0:1, :], 0.0, -1e30
        )

    keys = n_grp * seg_rows
    stat_copies = []
    part_copies = []
    for h in range(kv_heads):
        for copy in kv_copies[2 * h]:
            copy.wait_recv()
        hi, mid, low = split3(arrived[2 * h].reshape(keys, dim))
        kcat_a[:, :dim] = hi
        kcat_a[:, dim:] = mid
        kcat_b[:, :dim] = hi
        kcat_b[:, dim:] = low

        stats_out[h] = jnp.zeros_like(stats_out[h])

        def score(j, _, h=h):
            at = pl.ds(pl.multiple_of((h * group + j) * dim, dim), dim)
            q = queries[:, :, at].reshape(lanes, dim)
            hi, mid, low = split3(q)
            s = lax.dot_general(
                kcat_a[...], jnp.concatenate([hi, hi], 1), NT, preferred_element_type=F32
            )
            t = lax.dot_general(
                kcat_a[...], jnp.concatenate([mid, mid], 1), NT, preferred_element_type=F32
            )
            u = lax.dot_general(
                kcat_b[...], jnp.concatenate([low, hi], 1), NT, preferred_element_type=F32
            )
            b = bias[...]
            if lanes > 128:
                b = jnp.concatenate([b] * (lanes // 128), 1)
            s = (s + (t + u)) * scale + b
            peak = jnp.max(s, axis=0, keepdims=True)
            p = jnp.exp(s - peak)
            total = jnp.sum(p, axis=0, keepdims=True)
            hi = p.astype(BF16)
            p_hi[j] = hi
            p_lo[j] = (p - hi.astype(F32)).astype(BF16)
            stats_out[h, 0, pl.ds(j, 1), :] = peak
            stats_out[h, 1, pl.ds(j, 1), :] = total
            return 0

        lax.fori_loop(0, group, score, 0)
        row = []
        for e in range(1, n_blk):
            copy = pltpu.make_async_remote_copy(
                src_ref=stats_out.at[h],
                dst_ref=stats_in.at[h, e],
                send_sem=stat_send.at[h, e],
                recv_sem=stat_recv.at[h, e],
                device_id={"blk": lax.rem(me_b + e, n_blk)},
                device_id_type=MESH,
            )
            copy.start()
            row.append(copy)
        stat_copies.append(row)

        for copy in kv_copies[2 * h + 1]:
            copy.wait_recv()
        v = arrived[2 * h + 1].reshape(keys, dim).T
        hi = v.astype(BF16)
        v_t[:dim, :] = hi
        v_t[dim:, :] = (v - hi.astype(F32)).astype(BF16)
        for copy in row:
            copy.wait_recv()
        mine = stats_out[h, 0]
        top = mine
        for e in range(1, n_blk):
            top = jnp.maximum(top, stats_in[h, e, 0])
        factor = jnp.exp(mine - top)
        whole = stats_out[h, 1] * factor
        for e in range(1, n_blk):
            whole += stats_in[h, e, 1] * jnp.exp(stats_in[h, e, 0] - top)
        stats_in[h, 0, 0] = factor / whole

        def mix(j, _, h=h):
            o = dot(v_t[...], p_hi[j])
            o = o[:dim] + o[dim:] + dot(v_t[:dim, :], p_lo[j])
            o = (o * stats_in[h, 0, 0, pl.ds(j, 1), :]).T
            at = pl.ds(pl.multiple_of(j * dim, dim), dim)
            partial[h, :, :, at] = o.reshape(n_blk, rows, dim)
            return 0

        lax.fori_loop(0, group, mix, 0)
        row = []
        for e in range(1, n_blk):
            peer = lax.rem(me_b + e, n_blk)
            copy = pltpu.make_async_remote_copy(
                src_ref=partial.at[h, peer],
                dst_ref=partial_in.at[h, e - 1],
                send_sem=part_send.at[h, e],
                recv_sem=part_recv.at[h, e],
                device_id={"blk": peer},
                device_id_type=MESH,
            )
            copy.start()
            row.append(copy)
        part_copies.append(row)

    for h in range(kv_heads):
        for copy in part_copies[h]:
            copy.wait_recv()
        total = partial[h, me_b]
        for e in range(1, n_blk):
            total += partial_in[h, e - 1]
        out_ref[:, h * group * dim : (h + 1) * group * dim] = total

    for row in [query_copies, count_copies] + kv_copies + stat_copies + part_copies:
        for copy in row:
            copy.wait_send()


def on_device(n_grp, n_blk, visual, text_queries, kv_weight, placement):
    n_rows, model = visual.shape
    rows, wide = text_queries.shape
    dim = kv_weight.shape[1] // (2 * KV_HEADS)
    group = wide // dim // KV_HEADS
    blocks = placement.shape[0]
    block_rows = n_rows // blocks
    per_pair = max(2, blocks // (n_grp * n_blk) + 1)
    per_seg = n_blk * per_pair
    seg_rows = per_seg * block_rows
    keys = n_grp * seg_rows
    lanes = n_blk * rows
    heads = KV_HEADS
    units = 2 * heads
    stat_rows = -(-group // 8) * 8
    any_space = pl.BlockSpec(memory_space=pl.ANY)
    in_vmem = pl.BlockSpec(memory_space=pltpu.VMEM)
    dma = pltpu.SemaphoreType.DMA
    return pl.pallas_call(
        functools.partial(kernel, n_grp, n_blk, per_seg, group, dim),
        name="routed_attention",
        out_shape=jax.ShapeDtypeStruct((rows, wide), F32),
        in_specs=[any_space, any_space, any_space, in_vmem],
        out_specs=in_vmem,
        scratch_shapes=[
            pltpu.VMEM((n_rows, model), BF16),
            pltpu.VMEM((2, model, 2 * dim), BF16),
            pltpu.VMEM((n_rows, 6 * dim), BF16),
            pltpu.VMEM((units, n_grp, seg_rows, dim), F32),
            pltpu.VMEM((units, n_grp, seg_rows, dim), F32),
            pltpu.VMEM((n_blk, rows, wide), F32),
            pltpu.VMEM((n_grp, 8, 128), F32),
            pltpu.VMEM((n_grp, 8, 128), F32),
            pltpu.VMEM((keys, 128), F32),
            pltpu.VMEM((keys, 2 * dim), BF16),
            pltpu.VMEM((keys, 2 * dim), BF16),
            pltpu.VMEM((2 * dim, keys), BF16),
            pltpu.VMEM((group, keys, lanes), BF16),
            pltpu.VMEM((group, keys, lanes), BF16),
            pltpu.VMEM((heads, 2, stat_rows, lanes), F32),
            pltpu.VMEM((heads, n_blk, 2, stat_rows, lanes), F32),
            pltpu.VMEM((heads, n_blk, rows, group * dim), F32),
            pltpu.VMEM((heads, n_blk - 1, rows, group * dim), F32),
            dma,
            dma((2, 2)),
            dma,
            dma((n_blk,)),
            dma((n_blk,)),
            dma((n_grp,)),
            dma((n_grp,)),
            dma((units, n_grp)),
            dma((units, n_grp)),
            dma((heads, n_blk)),
            dma((heads, n_blk)),
            dma((heads, n_blk)),
            dma((heads, n_blk)),
        ],
        compiler_params=pltpu.CompilerParams(
            collective_id=0, has_side_effects=True, vmem_limit_bytes=67043328
        ),
    )(visual, text_queries, kv_weight, placement)


def solution(mesh):
    placed = (P(("grp", "blk"), None), P(("grp", "blk"), None), P(), P(("grp", "blk"), None))
    body = functools.partial(on_device, mesh.shape["grp"], mesh.shape["blk"])
    return jax.shard_map(
        body, mesh=mesh, in_specs=placed, out_specs=P(("grp", "blk"), None), check_vma=False
    )
```
